256 devices in a mesh: group: 32 (over z, y_hi, core), helper: 8 (over y_lo, x).
Axes of the slice: x: 4, y: 4 (y_hi: 2, y_lo: 2; y = y_hi * 2 + y_lo), z: 8, core: 2. Of those that a mesh axis runs over, the one named last changes fastest.
Arguments:
- candidates: bfloat16 [32, 2048, 1024], P('group', 'helper'), may hold values from -6 to 6
- prefix_cache: bfloat16 [32, 2, 3072, 1024], P('group', None, 'helper'), may hold values from -6 to 6
- w_uvqk: bfloat16 [1024, 4096], replicated, may hold values from -0.1875 to 0.1875
- w_output: bfloat16 [1024, 1024], replicated, may hold values from -0.1875 to 0.1875
- norm_gain: float32 [1024], replicated, may hold values from 0.1 to 1.9
- owner: int32 [32], replicated, may hold values from 0 to 31, as said below
- counts: int32 [32], replicated, may hold values from 1024 to 2048, as said below
- prefix_len: int32 [32], replicated, may hold values from 96 to 3072, as said below
Outputs:
- update: bfloat16 [32, 2048, 1024], P('group', 'helper')
The draws below stay inside these ranges and needn't reach their ends.
Inputs may be any that keep to these rules, and one draw needn't show every extreme that they name: owner[u] = (u + s) mod 32 for one shift s of the round. `counts`: multiples of 128; some user has exactly 2048. `prefix_len`: some user has exactly 3072.
All inputs are finite; a program needn't handle non-finite values.
Results may differ from the reference program's by a relative error of at most 0.012.
Values may be sent and summed in bfloat16 or wider, within the bound.
A program may use at most 128 MiB of HBM per device.

```python
import jax
import jax.numpy as jnp
from jax import lax

D = 1024
HEADS = 8
PREFIX = 3072
CAND = 2048
GRAIN = 128
USERS = 32


def draw_owner(key, part):
    offset = jax.random.randint(key, (), 0, USERS)
    return ((jnp.arange(USERS, dtype=jnp.int32) + offset) % USERS).astype(jnp.int32)


def draw_counts(key, part):
    first, second = jax.random.split(jax.random.fold_in(key, 11))
    steps = jax.random.randint(first, (USERS,), CAND // (2 * GRAIN), CAND // GRAIN + 1)
    chosen = jax.random.randint(second, (), 0, USERS)
    values = jnp.where(jnp.arange(USERS) == chosen, CAND, steps * GRAIN)
    return values.astype(jnp.int32)


def draw_prefix_len(key, part):
    first, second = jax.random.split(jax.random.fold_in(key, 23))
    values = jax.random.randint(first, (USERS,), max(1, PREFIX // 32), PREFIX + 1)
    chosen = jax.random.randint(second, (), 0, USERS)
    values = jnp.where(jnp.arange(USERS) == chosen, PREFIX, values)
    return values.astype(jnp.int32)


def block_levels(own_key, dims, shards, smallest, high):
    def one(position, blocks):
        draws = jax.random.uniform(jax.random.fold_in(jax.random.fold_in(own_key, 6), position), (blocks,), jnp.float32, smallest / len(shards), high / len(shards))
        return jnp.repeat(jnp.exp(draws), dims[position] // blocks).reshape((-1,) + (1,) * (len(dims) - position - 1))

    factor_of = one(*shards[0])
    for cut in shards[1:]:
        factor_of = factor_of * one(*cut)
    return factor_of


def noise(stream_key, shape, scale, most, cuts=(), kind=jnp.bfloat16):
    level = block_levels(stream_key, shape, cuts, -0.22, 0.18) if cuts else 1.0
    values = jax.random.normal(stream_key, shape, jnp.float32) * scale * level
    return jnp.minimum(jnp.maximum(values, -most), most).astype(kind)


def setup_inputs(seed: int = 0) -> dict:
    seeds = jax.random.split(jax.random.key(seed), 9)
    candidates = noise(seeds[0], (USERS, CAND, D), 1.0, 6.0, ((0, 32), (1, 8)))
    prefix_cache = noise(seeds[1], (USERS, 2, PREFIX, D), 1.0, 6.0, ((0, 32), (2, 8)))
    w_uvqk = noise(seeds[2], (D, 4 * D), D ** -0.5, 0.1875)
    w_output = noise(seeds[3], (D, D), D ** -0.5, 0.1875)
    norm_gain = jnp.clip(1.0 + 0.18 * jax.random.normal(seeds[4], (D,), jnp.float32), 0.1, 1.9)
    owner = draw_owner(jax.random.fold_in(seeds[8], 71), 0)
    counts = draw_counts(jax.random.fold_in(seeds[8], 71), 0)
    prefix_len = draw_prefix_len(jax.random.fold_in(seeds[8], 71), 0)
    return dict(candidates=candidates, prefix_cache=prefix_cache, w_uvqk=w_uvqk, w_output=w_output, norm_gain=norm_gain, owner=owner, counts=counts, prefix_len=prefix_len)


def score_user(rows, keys, values, count, visible, w_uvqk, w_output, norm_gain):
    width = rows.shape[1]
    head = width // HEADS
    scale = head ** (-0.5)
    total = rows.shape[0]
    proj = jax.nn.silu(jnp.dot(rows, w_uvqk, preferred_element_type=jnp.float32))
    gate_u = proj[:, :width]
    own_v = proj[:, width:2 * width].astype(jnp.bfloat16).astype(jnp.float32).reshape(total, HEADS, head)
    query = proj[:, 2 * width:3 * width].astype(jnp.bfloat16).astype(jnp.float32).reshape(total, HEADS, head)
    own_k = proj[:, 3 * width:].astype(jnp.bfloat16).astype(jnp.float32).reshape(total, HEADS, head)
    length = keys.shape[0]
    keys4 = keys.astype(jnp.float32).reshape(length, HEADS, head)
    values4 = values.astype(jnp.float32).reshape(length, HEADS, head)
    scores = jnp.einsum('rhd,nhd->hrn', query, keys4) * scale
    allowed = jnp.arange(length, dtype=jnp.int32) < visible
    weights = jnp.where(allowed[None, None, :], jax.nn.silu(scores), 0.0).astype(jnp.bfloat16).astype(jnp.float32)
    mixed = jnp.einsum('hrn,nhd->rhd', weights, values4)
    selfw = jax.nn.silu(lax.optimization_barrier(jnp.sum(query * own_k, axis=-1)) * scale).astype(jnp.bfloat16).astype(jnp.float32)
    mixed = (mixed + selfw[:, :, None] * own_v).reshape(total, width)
    centre = mixed - lax.optimization_barrier(jnp.mean(mixed, axis=-1, keepdims=True))
    spread = lax.optimization_barrier(jnp.mean(centre * centre, axis=-1, keepdims=True))
    normed = (centre * lax.rsqrt(spread + 1e-05) * norm_gain * gate_u).astype(jnp.bfloat16)
    result = jnp.dot(normed, w_output, preferred_element_type=jnp.float32)
    live = jnp.arange(total, dtype=jnp.int32) < count
    return jnp.where(live[:, None], result, 0.0).astype(jnp.bfloat16)

def reference(candidates, prefix_cache, w_uvqk, w_output, norm_gain, owner, counts, prefix_len):
    shift = owner[0]

    def one_user(user):
        rows = lax.dynamic_index_in_dim(candidates, user, 0, keepdims=False)
        source = ((user + shift) % USERS).astype(jnp.int32)
        cache = lax.dynamic_index_in_dim(prefix_cache, source, 0, keepdims=False)
        count = lax.dynamic_index_in_dim(counts, user, 0, keepdims=False)
        visible = lax.dynamic_index_in_dim(prefix_len, user, 0, keepdims=False)
        return score_user(rows, cache[0], cache[1], count, visible, w_uvqk, w_output, norm_gain)
    result = lax.map(one_user, jnp.arange(USERS, dtype=jnp.int32))
    return jnp.roll(result, shift, axis=0)
```

```python
import functools
import math

import jax
import jax.numpy as jnp
from jax import lax
from jax.sharding import PartitionSpec as P

HEADS = 8


def from_behind(value, axis, steps):
    if steps == 0:
        return value
    count = lax.axis_size(axis)
    pairs = [(source, (source + steps) % count) for source in range(count)]
    return lax.ppermute(value, axis, pairs)


def pick(table, index):
    places = jnp.arange(table.shape[0], dtype=jnp.int32)
    return jnp.sum(jnp.where(places == index, table, 0))


def local(candidates, prefix_cache, w_uvqk, w_output, norm_gain, owner, counts, prefix_len):
    groups = lax.axis_size("group")
    helpers = lax.axis_size("helper")
    group_here = lax.axis_index("group")
    helper_here = lax.axis_index("helper")
    offset = owner[0]
    slots = candidates.shape[1]
    width = candidates.shape[2]
    head = width // HEADS
    scale = head ** (-0.5)
    branches = [functools.partial(from_behind, axis="group", steps=steps) for steps in range(groups)]
    tokens = lax.switch(offset, branches, candidates[0])
    user = (group_here - offset) % groups
    count = pick(counts, user)
    visible = pick(prefix_len, user)
    live = jnp.clip(count - helper_here * slots, 0, slots)
    proj = jax.nn.silu(jnp.dot(tokens, w_uvqk, preferred_element_type=jnp.float32))
    gate_u = proj[:, :width]
    own_v = proj[:, width : 2 * width].astype(jnp.bfloat16).reshape(slots, HEADS, head)
    query = proj[:, 2 * width : 3 * width].astype(jnp.bfloat16).reshape(slots, HEADS, head)
    own_k = proj[:, 3 * width :].astype(jnp.bfloat16).reshape(slots, HEADS, head)
    local_heads = HEADS // helpers
    local_width = width // helpers
    parts = lax.all_to_all(prefix_cache, "helper", split_axis=3, concat_axis=2, tiled=True)
    query_cols = lax.all_to_all(
        query.reshape(slots, width), "helper", split_axis=1, concat_axis=0, tiled=True
    )
    rows_all = query_cols.shape[0]
    length = parts.shape[2]
    keys_heads = parts[0, 0].reshape(length, local_heads, head)
    values_heads = parts[0, 1].reshape(length, local_heads, head)
    allowed_all = jnp.arange(length, dtype=jnp.int32) < visible
    big = math.gcd(rows_all, 512)
    blocks_heads = (jnp.minimum(count, rows_all) + big - 1) // big

    def head_block(number, acc):
        first = number * big
        query_block = lax.dynamic_slice_in_dim(query_cols, first, big, 0).reshape(
            big, local_heads, head
        )
        scores = (
            jnp.einsum("rhd,nhd->hrn", query_block, keys_heads, preferred_element_type=jnp.float32)
            * scale
        )
        weights = jnp.where(allowed_all[None, None, :], jax.nn.silu(scores), 0.0).astype(
            jnp.bfloat16
        )
        partial_block = jnp.einsum(
            "hrn,nhd->rhd", weights, values_heads, preferred_element_type=jnp.float32
        )
        return lax.dynamic_update_slice_in_dim(
            acc, partial_block.reshape(big, local_width), first, 0
        )

    heads_out = lax.fori_loop(
        0, blocks_heads, head_block, jnp.zeros((rows_all, local_width), jnp.float32)
    )
    mixed = lax.all_to_all(
        heads_out.astype(jnp.bfloat16), "helper", split_axis=0, concat_axis=1, tiled=True
    ).astype(heads_out.dtype)
    selfw = jax.nn.silu(
        jnp.einsum("rhd,rhd->rh", query, own_k, preferred_element_type=jnp.float32) * scale
    ).astype(jnp.bfloat16)
    mixed = mixed + (selfw.astype(jnp.float32)[:, :, None] * own_v.astype(jnp.float32)).reshape(
        slots, width
    )
    centre = mixed - jnp.mean(mixed, axis=-1, keepdims=True)
    spread = jnp.mean(centre * centre, axis=-1, keepdims=True)
    normed = (centre * lax.rsqrt(spread + 1e-05) * norm_gain * gate_u).astype(jnp.bfloat16)
    result = jnp.dot(normed, w_output, preferred_element_type=jnp.float32)
    alive = jnp.arange(slots, dtype=jnp.int32) < live
    result = jnp.where(alive[:, None], result, 0.0).astype(jnp.bfloat16)
    return result[None]


def solution(mesh):
    in_specs = (
        P("group", "helper", None),
        P("group", None, "helper", None),
        P(),
        P(),
        P(),
        P(),
        P(),
        P(),
    )
    out_specs = P("group", "helper", None)
    return jax.shard_map(local, mesh=mesh, in_specs=in_specs, out_specs=out_specs, check_vma=False)
```

```python
import functools
import math

import jax
import jax.numpy as jnp
from jax import lax
from jax.experimental import pallas as pl
from jax.experimental.pallas import tpu as pltpu
from jax.sharding import PartitionSpec as P

HEADS = 8
RUN = 4
COLUMNS = 512
KEYS = 256
MESH = pl.DeviceIdType.MESH


def from_behind(value, axis, steps):
    if steps == 0:
        return value
    count = lax.axis_size(axis)
    pairs = [(source, (source + steps) % count) for source in range(count)]
    return lax.ppermute(value, axis, pairs)


def near(me, step):
    row = lax.rem(me // RUN + step // RUN, HEADS // RUN)
    place = lax.rem(lax.rem(me, RUN) + lax.rem(step, RUN), RUN)
    return row * RUN + place


def back(me, step):
    row = lax.rem(me // RUN + step // RUN, HEADS // RUN)
    place = lax.rem(lax.rem(me, RUN) + RUN - lax.rem(step, RUN), RUN)
    return row * RUN + place


def silu(value):
    half = 0.5 * value
    return half + half * jnp.tanh(half)


def score(
    owner_ref,
    counts_ref,
    visible_ref,
    tokens_hbm,
    prefix_hbm,
    w_hbm,
    w_output_hbm,
    gain_ref,
    out_ref,
    tokens,
    keys,
    values,
    w,
    w_output,
    query_out,
    query_in,
    mixed_out,
    mixed_in,
    gate,
    own,
    normed,
    load_sem,
    query_send,
    query_recv,
    mixed_send,
    mixed_recv,
):
    me = lax.axis_index("helper")
    group = lax.axis_index("group")
    users = lax.axis_size("group")
    slots, width = tokens.shape
    head = width // HEADS
    length = keys.shape[0]
    scale = head ** (-0.5)

    def load(number, source, target):
        copy = pltpu.make_async_copy(source, target, load_sem.at[number])
        copy.start()
        return copy

    load_tokens = load(0, tokens_hbm, tokens)
    parts = [2, 0, 1, 3]
    load_w = [
        load(1 + at, w_hbm.at[:, pl.ds(part * width, width)], w.at[part])
        for at, part in enumerate(parts)
    ]
    load_keys = load(5, prefix_hbm.at[0], keys)
    load_values = load(6, prefix_hbm.at[1], values)
    load_output = load(7, w_output_hbm, w_output)

    barrier = pltpu.get_barrier_semaphore()
    for step in range(1, HEADS):
        pl.semaphore_signal(
            barrier, inc=1, device_id={"helper": near(me, step)}, device_id_type=MESH
        )
    pl.semaphore_wait(barrier, HEADS - 1)

    def send_query(step):
        peer = near(me, step)
        return pltpu.make_async_remote_copy(
            src_ref=query_out.at[peer],
            dst_ref=query_in.at[me],
            send_sem=query_send.at[step],
            recv_sem=query_recv.at[step],
            device_id={"helper": peer},
            device_id_type=MESH,
        )

    def send_mixed(step):
        peer = back(me, step)
        return pltpu.make_async_remote_copy(
            src_ref=mixed_out.at[step],
            dst_ref=mixed_in.at[me],
            send_sem=mixed_send.at[step],
            recv_sem=mixed_recv.at[step],
            device_id={"helper": peer},
            device_id_type=MESH,
        )

    def project(part, at, columns):
        return silu(
            jnp.dot(
                tokens[...],
                w[part, :, at * columns : (at + 1) * columns],
                preferred_element_type=jnp.float32,
            )
        )

    per = COLUMNS // head
    load_tokens.wait()
    load_w[0].wait()
    for at in range(width // COLUMNS):
        block = project(2, at, COLUMNS).astype(jnp.bfloat16)
        for number in range(per):
            query_out[at * per + number] = block[:, number * head : (number + 1) * head]
    query_in[me] = query_out[me]
    for step in range(1, HEADS):
        send_query(step).start()

    for copy in load_w[1:]:
        copy.wait()
    for at in range(width // COLUMNS):
        columns = slice(at * COLUMNS, (at + 1) * COLUMNS)
        gate[:, columns] = project(0, at, COLUMNS)
        own_v = project(1, at, COLUMNS).astype(jnp.bfloat16).astype(jnp.float32)
        own_k = project(3, at, COLUMNS).astype(jnp.bfloat16).astype(jnp.float32)
        for number in range(per):
            part = slice(number * head, (number + 1) * head)
            query = query_out[at * per + number].astype(jnp.float32)
            weight = silu(jnp.sum(query * own_k[:, part], axis=-1, keepdims=True) * scale)
            weight = weight.astype(jnp.bfloat16).astype(jnp.float32)
            own[at * per + number] = weight * own_v[:, part]

    user = lax.rem(group - owner_ref[0] + users, users)
    count = counts_ref[user]
    visible = visible_ref[user]

    load_keys.wait()
    load_values.wait()
    place = lax.broadcasted_iota(jnp.int32, (length, head), 0)
    values[...] = jnp.where(place < visible, values[...], jnp.zeros_like(values[...]))

    def attend(query):
        total = jnp.zeros((slots, head), jnp.float32)
        for at in range(length // KEYS):
            chosen = slice(at * KEYS, (at + 1) * KEYS)
            scores = lax.dot_general(
                query,
                keys[chosen],
                (((1,), (1,)), ((), ())),
                preferred_element_type=jnp.float32,
            )
            weights = silu(scores * scale).astype(jnp.bfloat16)
            total += jnp.dot(weights, values[chosen], preferred_element_type=jnp.float32)
        return total.astype(jnp.bfloat16)

    mixed_in[me] = attend(query_in[me])

    def visit(step, carry):
        send_query(step).wait_recv()
        mixed_out[step] = attend(query_in[back(me, step)])
        send_mixed(step).start()
        return carry

    lax.fori_loop(1, HEADS, visit, 0)

    for step in range(1, HEADS):
        send_query(step).wait_send()
        send_mixed(step).wait()
    load_output.wait()

    total = jnp.zeros((slots, 1), jnp.float32)
    for number in range(HEADS):
        piece = mixed_in[number].astype(jnp.float32) + own[number]
        own[number] = piece
        total += jnp.sum(piece, axis=-1, keepdims=True)
    mean = total / width
    total = jnp.zeros((slots, 1), jnp.float32)
    for number in range(HEADS):
        piece = own[number] - mean
        total += jnp.sum(piece * piece, axis=-1, keepdims=True)
    factor = lax.rsqrt(total / width + 1e-05)
    for number in range(HEADS):
        part = slice(number * head, (number + 1) * head)
        normed[:, part] = (
            (own[number] - mean) * factor * gain_ref[:, part] * gate[:, part]
        ).astype(jnp.bfloat16)
    live = count - me * slots
    row = lax.broadcasted_iota(jnp.int32, (slots, COLUMNS), 0)
    for at in range(width // COLUMNS):
        columns = slice(at * COLUMNS, (at + 1) * COLUMNS)
        result = jnp.dot(normed[...], w_output[:, columns], preferred_element_type=jnp.float32)
        out_ref[:, columns] = jnp.where(row < live, result, 0.0).astype(jnp.bfloat16)


def score_call(tokens, prefix, w_uvqk, w_output, norm_gain, owner, counts, prefix_len):
    slots, width = tokens.shape
    head = width // HEADS
    length = prefix.shape[1]
    smem = pl.BlockSpec(memory_space=pltpu.SMEM)
    hbm = pl.BlockSpec(memory_space=pl.ANY)
    vmem = pl.BlockSpec(memory_space=pltpu.VMEM)
    bf16, f32 = jnp.bfloat16, jnp.float32
    return pl.pallas_call(
        score,
        out_shape=jax.ShapeDtypeStruct((slots, width), bf16),
        in_specs=[smem, smem, smem, hbm, hbm, hbm, hbm, vmem],
        out_specs=vmem,
        scratch_shapes=[
            pltpu.VMEM((slots, width), bf16),
            pltpu.VMEM((length, head), bf16),
            pltpu.VMEM((length, head), bf16),
            pltpu.VMEM((4, width, width), bf16),
            pltpu.VMEM((width, width), bf16),
            pltpu.VMEM((HEADS, slots, head), bf16),
            pltpu.VMEM((HEADS, slots, head), bf16),
            pltpu.VMEM((HEADS, slots, head), bf16),
            pltpu.VMEM((HEADS, slots, head), bf16),
            pltpu.VMEM((slots, width), f32),
            pltpu.VMEM((HEADS, slots, head), f32),
            pltpu.VMEM((slots, width), bf16),
            pltpu.SemaphoreType.DMA((8,)),
            pltpu.SemaphoreType.DMA((HEADS,)),
            pltpu.SemaphoreType.DMA((HEADS,)),
            pltpu.SemaphoreType.DMA((HEADS,)),
            pltpu.SemaphoreType.DMA((HEADS,)),
        ],
        compiler_params=pltpu.CompilerParams(
            collective_id=0, has_side_effects=True, vmem_limit_bytes=48 * 1024 * 1024
        ),
        name="score",
    )(
        owner,
        counts,
        prefix_len,
        tokens,
        prefix,
        w_uvqk,
        w_output,
        norm_gain.reshape(1, width),
    )


def local(candidates, prefix_cache, w_uvqk, w_output, norm_gain, owner, counts, prefix_len):
    groups = lax.axis_size("group")
    branches = [functools.partial(from_behind, axis="group", steps=steps) for steps in range(groups)]
    tokens = lax.switch(owner[0], branches, candidates[0])
    prefix = lax.all_to_all(prefix_cache, "helper", split_axis=3, concat_axis=2, tiled=True)[0]
    return score_call(
        tokens, prefix, w_uvqk, w_output, norm_gain, owner, counts, prefix_len
    )[None]


def solution(mesh):
    in_specs = (
        P("group", "helper", None),
        P("group", None, "helper", None),
        P(),
        P(),
        P(),
        P(),
        P(),
        P(),
    )
    out_specs = P("group", "helper", None)
    return jax.shard_map(local, mesh=mesh, in_specs=in_specs, out_specs=out_specs, check_vma=False)
```

```python
import functools
import math

import jax
import jax.numpy as jnp
from jax import lax
from jax.experimental import pallas as pl
from jax.experimental.pallas import tpu as pltpu
from jax.sharding import PartitionSpec as P

HEADS = 8
RUN = 4
COLUMNS = 512
KEYS = 256
MESH = pl.DeviceIdType.MESH


def near(me, step):
    row = lax.rem(me // RUN + step // RUN, HEADS // RUN)
    place = lax.rem(lax.rem(me, RUN) + lax.rem(step, RUN), RUN)
    return row * RUN + place


def back(me, step):
    row = lax.rem(me // RUN + step // RUN, HEADS // RUN)
    place = lax.rem(lax.rem(me, RUN) + RUN - lax.rem(step, RUN), RUN)
    return row * RUN + place


def silu(value):
    half = 0.5 * value
    return half + half * jnp.tanh(half)


def score(
    owner_ref,
    counts_ref,
    visible_ref,
    tokens_hbm,
    prefix_hbm,
    w_hbm,
    w_output_hbm,
    gain_ref,
    out_ref,
    tokens,
    keys,
    values,
    w,
    w_output,
    query_out,
    query_in,
    mixed_out,
    mixed_in,
    gate,
    own,
    normed,
    load_sem,
    query_send,
    query_recv,
    mixed_send,
    mixed_recv,
):
    me = lax.axis_index("helper")
    group = lax.axis_index("group")
    users = lax.axis_size("group")
    slots, width = tokens.shape
    head = width // HEADS
    length = keys.shape[0]
    scale = head ** (-0.5)

    def load(number, source, target):
        copy = pltpu.make_async_copy(source, target, load_sem.at[number])
        copy.start()
        return copy

    load_tokens = load(0, tokens_hbm, tokens)
    parts = [2, 0, 1, 3]
    load_w = [
        load(1 + at, w_hbm.at[:, pl.ds(part * width, width)], w.at[part])
        for at, part in enumerate(parts)
    ]
    load_keys = load(5, prefix_hbm.at[0], keys)
    load_values = load(6, prefix_hbm.at[1], values)
    load_output = load(7, w_output_hbm, w_output)

    barrier = pltpu.get_barrier_semaphore()
    for step in range(1, HEADS):
        pl.semaphore_signal(
            barrier, inc=1, device_id={"helper": near(me, step)}, device_id_type=MESH
        )
    pl.semaphore_wait(barrier, HEADS - 1)

    def send_query(step):
        peer = near(me, step)
        return pltpu.make_async_remote_copy(
            src_ref=query_out.at[peer],
            dst_ref=query_in.at[me],
            send_sem=query_send.at[step],
            recv_sem=query_recv.at[step],
            device_id={"helper": peer},
            device_id_type=MESH,
        )

    def send_mixed(step):
        peer = back(me, step)
        return pltpu.make_async_remote_copy(
            src_ref=mixed_out.at[step],
            dst_ref=mixed_in.at[me],
            send_sem=mixed_send.at[step],
            recv_sem=mixed_recv.at[step],
            device_id={"helper": peer},
            device_id_type=MESH,
        )

    def project(part, at, columns):
        return silu(
            jnp.dot(
                tokens[...],
                w[part, :, at * columns : (at + 1) * columns],
                preferred_element_type=jnp.float32,
            )
        )

    per = COLUMNS // head
    load_tokens.wait()
    load_w[0].wait()
    for at in range(width // COLUMNS):
        block = project(2, at, COLUMNS).astype(jnp.bfloat16)
        for number in range(per):
            query_out[at * per + number] = block[:, number * head : (number + 1) * head]
    query_in[me] = query_out[me]
    for step in range(1, HEADS):
        send_query(step).start()

    for copy in load_w[1:]:
        copy.wait()
    for at in range(width // COLUMNS):
        columns = slice(at * COLUMNS, (at + 1) * COLUMNS)
        gate[:, columns] = project(0, at, COLUMNS)
        own_v = project(1, at, COLUMNS).astype(jnp.bfloat16).astype(jnp.float32)
        own_k = project(3, at, COLUMNS).astype(jnp.bfloat16).astype(jnp.float32)
        for number in range(per):
            part = slice(number * head, (number + 1) * head)
            query = query_out[at * per + number].astype(jnp.float32)
            weight = silu(jnp.sum(query * own_k[:, part], axis=-1, keepdims=True) * scale)
            weight = weight.astype(jnp.bfloat16).astype(jnp.float32)
            own[at * per + number] = weight * own_v[:, part]

    user = lax.rem(group - owner_ref[0] + users, users)
    count = counts_ref[user]
    visible = visible_ref[user]

    load_keys.wait()
    load_values.wait()
    place = lax.broadcasted_iota(jnp.int32, (length, head), 0)
    values[...] = jnp.where(place < visible, values[...], jnp.zeros_like(values[...]))

    def attend(query):
        total = jnp.zeros((slots, head), jnp.float32)
        for at in range(length // KEYS):
            chosen = slice(at * KEYS, (at + 1) * KEYS)
            scores = lax.dot_general(
                query,
                keys[chosen],
                (((1,), (1,)), ((), ())),
                preferred_element_type=jnp.float32,
            )
            weights = silu(scores * scale).astype(jnp.bfloat16)
            total += jnp.dot(weights, values[chosen], preferred_element_type=jnp.float32)
        return total.astype(jnp.bfloat16)

    mixed_in[me] = attend(query_in[me])

    def visit(step, carry):
        send_query(step).wait_recv()
        mixed_out[step] = attend(query_in[back(me, step)])
        send_mixed(step).start()
        return carry

    lax.fori_loop(1, HEADS, visit, 0)

    for step in range(1, HEADS):
        send_query(step).wait_send()
        send_mixed(step).wait()
    load_output.wait()

    total = jnp.zeros((slots, 1), jnp.float32)
    for number in range(HEADS):
        piece = mixed_in[number].astype(jnp.float32) + own[number]
        own[number] = piece
        total += jnp.sum(piece, axis=-1, keepdims=True)
    mean = total / width
    total = jnp.zeros((slots, 1), jnp.float32)
    for number in range(HEADS):
        piece = own[number] - mean
        total += jnp.sum(piece * piece, axis=-1, keepdims=True)
    factor = lax.rsqrt(total / width + 1e-05)
    for number in range(HEADS):
        part = slice(number * head, (number + 1) * head)
        normed[:, part] = (
            (own[number] - mean) * factor * gain_ref[:, part] * gate[:, part]
        ).astype(jnp.bfloat16)
    live = count - me * slots
    row = lax.broadcasted_iota(jnp.int32, (slots, COLUMNS), 0)
    for at in range(width // COLUMNS):
        columns = slice(at * COLUMNS, (at + 1) * COLUMNS)
        result = jnp.dot(normed[...], w_output[:, columns], preferred_element_type=jnp.float32)
        out_ref[:, columns] = jnp.where(row < live, result, 0.0).astype(jnp.bfloat16)


def score_call(tokens, prefix, w_uvqk, w_output, norm_gain, owner, counts, prefix_len):
    slots, width = tokens.shape
    head = width // HEADS
    length = prefix.shape[1]
    smem = pl.BlockSpec(memory_space=pltpu.SMEM)
    hbm = pl.BlockSpec(memory_space=pl.ANY)
    vmem = pl.BlockSpec(memory_space=pltpu.VMEM)
    bf16, f32 = jnp.bfloat16, jnp.float32
    return pl.pallas_call(
        score,
        out_shape=jax.ShapeDtypeStruct((slots, width), bf16),
        in_specs=[smem, smem, smem, hbm, hbm, hbm, hbm, vmem],
        out_specs=vmem,
        scratch_shapes=[
            pltpu.VMEM((slots, width), bf16),
            pltpu.VMEM((length, head), bf16),
            pltpu.VMEM((length, head), bf16),
            pltpu.VMEM((4, width, width), bf16),
            pltpu.VMEM((width, width), bf16),
            pltpu.VMEM((HEADS, slots, head), bf16),
            pltpu.VMEM((HEADS, slots, head), bf16),
            pltpu.VMEM((HEADS, slots, head), bf16),
            pltpu.VMEM((HEADS, slots, head), bf16),
            pltpu.VMEM((slots, width), f32),
            pltpu.VMEM((HEADS, slots, head), f32),
            pltpu.VMEM((slots, width), bf16),
            pltpu.SemaphoreType.DMA((8,)),
            pltpu.SemaphoreType.DMA((HEADS,)),
            pltpu.SemaphoreType.DMA((HEADS,)),
            pltpu.SemaphoreType.DMA((HEADS,)),
            pltpu.SemaphoreType.DMA((HEADS,)),
        ],
        compiler_params=pltpu.CompilerParams(
            collective_id=0, has_side_effects=True, vmem_limit_bytes=48 * 1024 * 1024
        ),
        name="score",
    )(
        owner,
        counts,
        prefix_len,
        tokens,
        prefix,
        w_uvqk,
        w_output,
        norm_gain.reshape(1, width),
    )


def move(shift, users, rows_hbm, cache_hbm, tokens_hbm, prefix_hbm, kept, kept_rows, row_sems, cache_send, cache_recv, own_sem):
    me = lax.axis_index("helper")
    group = lax.axis_index("group")
    length, width = cache_hbm.shape[2:]
    head = width // HEADS
    ahead = lax.rem(group + shift, users)
    behind = lax.rem(group + users - shift, users)

    def send_cache(step, part):
        peer = near(me, step)
        return pltpu.make_async_remote_copy(
            src_ref=cache_hbm.at[0, part, :, pl.ds(pl.multiple_of(peer * head, head), head)],
            dst_ref=prefix_hbm.at[part, pl.ds(pl.multiple_of(me * length, length), length)],
            send_sem=cache_send.at[step, part],
            recv_sem=cache_recv.at[step, part],
            device_id={"helper": peer},
            device_id_type=MESH,
        )

    if shift:
        send_rows = pltpu.make_async_remote_copy(
            src_ref=rows_hbm.at[0],
            dst_ref=tokens_hbm,
            send_sem=row_sems.at[0],
            recv_sem=row_sems.at[1],
            device_id={"group": ahead},
            device_id_type=MESH,
        )
    else:
        keep_rows = pltpu.make_async_copy(rows_hbm.at[0], kept_rows, row_sems.at[0])
        put_rows = pltpu.make_async_copy(kept_rows, tokens_hbm, row_sems.at[1])
        keep_rows.start()
    keep = pltpu.make_async_copy(
        cache_hbm.at[0, :, :, pl.ds(pl.multiple_of(me * head, head), head)], kept, own_sem.at[0]
    )
    put = pltpu.make_async_copy(
        kept, prefix_hbm.at[:, pl.ds(pl.multiple_of(me * length, length), length)], own_sem.at[1]
    )
    keep.start()
    barrier = pltpu.get_barrier_semaphore()
    for step in range(1, HEADS):
        pl.semaphore_signal(
            barrier, inc=1, device_id={"helper": near(me, step)}, device_id_type=MESH
        )
    if shift:
        for peer in (ahead, behind):
            pl.semaphore_signal(barrier, inc=1, device_id={"group": peer}, device_id_type=MESH)
    pl.semaphore_wait(barrier, HEADS + 1 if shift else HEADS - 1)
    if shift:
        send_rows.start()
    for step in range(1, HEADS):
        for part in range(2):
            send_cache(step, part).start()
    if not shift:
        keep_rows.wait()
        put_rows.start()
        put_rows.wait()
    keep.wait()
    put.start()
    put.wait()
    for step in range(1, HEADS):
        for part in range(2):
            send_cache(step, part).wait()
    if shift:
        send_rows.wait()


def move_call(shift, users, rows, cache):
    slots, width = rows.shape[1:]
    length = cache.shape[2]
    head = width // HEADS
    hbm = pl.BlockSpec(memory_space=pl.ANY)
    return pl.pallas_call(
        functools.partial(move, shift, users),
        out_shape=(
            jax.ShapeDtypeStruct((slots, width), rows.dtype),
            jax.ShapeDtypeStruct((2, HEADS * length, head), cache.dtype),
        ),
        in_specs=[hbm, hbm],
        out_specs=(hbm, hbm),
        scratch_shapes=[
            pltpu.VMEM((2, length, head), cache.dtype),
            pltpu.VMEM((slots, width), rows.dtype),
            pltpu.SemaphoreType.DMA((2,)),
            pltpu.SemaphoreType.DMA((HEADS, 2)),
            pltpu.SemaphoreType.DMA((HEADS, 2)),
            pltpu.SemaphoreType.DMA((2,)),
        ],
        compiler_params=pltpu.CompilerParams(collective_id=1 + shift, has_side_effects=True),
        name=f"move{shift}",
    )(rows, cache)


def local(candidates, prefix_cache, w_uvqk, w_output, norm_gain, owner, counts, prefix_len):
    users = lax.axis_size("group")
    branches = [functools.partial(move_call, shift, users) for shift in range(users)]
    tokens, prefix = lax.switch(owner[0], branches, candidates, prefix_cache)
    return score_call(
        tokens, prefix, w_uvqk, w_output, norm_gain, owner, counts, prefix_len
    )[None]


def solution(mesh):
    in_specs = (
        P("group", "helper", None),
        P("group", None, "helper", None),
        P(),
        P(),
        P(),
        P(),
        P(),
        P(),
    )
    out_specs = P("group", "helper", None)
    return jax.shard_map(local, mesh=mesh, in_specs=in_specs, out_specs=out_specs, check_vma=False)
```

```python
import functools
import math

import jax
import jax.numpy as jnp
from jax import lax
from jax.experimental import pallas as pl
from jax.experimental.pallas import tpu as pltpu
from jax.sharding import PartitionSpec as P

HEADS = 8
RUN = 4
COLUMNS = 512
KEYS = 256
GROUPS = 4
PIECES = 8
ORDER = (6, 2, 5, 7, 1, 3, 4)
LEAP = 3
MESH = pl.DeviceIdType.MESH


def near(me, step):
    row = lax.rem(me // RUN + step // RUN, HEADS // RUN)
    place = lax.rem(lax.rem(me, RUN) + lax.rem(step, RUN), RUN)
    return row * RUN + place


def back(me, step):
    row = lax.rem(me // RUN + step // RUN, HEADS // RUN)
    place = lax.rem(lax.rem(me, RUN) + RUN - lax.rem(step, RUN), RUN)
    return row * RUN + place


def nth(turn):
    step = ORDER[0]
    for number in range(1, len(ORDER)):
        step = jnp.where(turn == number, ORDER[number], step)
    return step


def silu(value):
    half = 0.5 * value
    return half + half * jnp.tanh(half)


def score(
    owner_ref,
    counts_ref,
    visible_ref,
    tokens,
    query_in,
    own_query_hbm,
    prefix_hbm,
    w_hbm,
    w_output,
    gain_ref,
    out_ref,
    keys,
    values,
    across,
    w,
    own_query,
    mixed_out,
    mixed_in,
    gate,
    own,
    normed,
    load_sem,
    mixed_send,
    mixed_recv,
):
    me = lax.axis_index("helper")
    group = lax.axis_index("group")
    users = lax.axis_size("group")
    slots, width = tokens.shape
    head = width // HEADS
    length = keys.shape[0]
    scale = head ** (-0.5)

    def load(number, source, target):
        copy = pltpu.make_async_copy(source, target, load_sem.at[number])
        copy.start()
        return copy

    load_keys = load(0, prefix_hbm.at[0], keys)
    load_values = load(1, prefix_hbm.at[1], values)
    load_own = load(5, own_query_hbm, own_query)
    load_w = [
        load(2 + at, w_hbm.at[:, pl.ds(part * width, width)], w.at[at])
        for at, part in enumerate((0, 1, 3))
    ]

    barrier = pltpu.get_barrier_semaphore()
    for step in range(1, HEADS):
        pl.semaphore_signal(
            barrier, inc=1, device_id={"helper": near(me, step)}, device_id_type=MESH
        )

    def send_mixed(step):
        peer = back(me, step)
        return pltpu.make_async_remote_copy(
            src_ref=mixed_out.at[step],
            dst_ref=mixed_in.at[me],
            send_sem=mixed_send.at[step],
            recv_sem=mixed_recv.at[step],
            device_id={"helper": peer},
            device_id_type=MESH,
        )

    def project(part, at):
        return silu(
            jnp.dot(
                tokens[...],
                w[part, :, at * COLUMNS : (at + 1) * COLUMNS],
                preferred_element_type=jnp.float32,
            )
        )

    user = lax.rem(group - owner_ref[0] + users, users)
    count = counts_ref[user]
    visible = visible_ref[user]

    def attend(query):
        total = jnp.zeros((head, slots), jnp.float32)
        for at in range(length // KEYS):
            chosen = slice(at * KEYS, (at + 1) * KEYS)
            scores = lax.dot_general(
                keys[chosen],
                query,
                (((1,), (1,)), ((), ())),
                preferred_element_type=jnp.float32,
            )
            weights = silu(scores * scale).astype(jnp.bfloat16)
            total += jnp.dot(across[:, chosen], weights, preferred_element_type=jnp.float32)
        return total.T.astype(jnp.bfloat16)

    load_keys.wait()
    load_values.wait()
    for at in range(length // COLUMNS):
        chosen = slice(at * COLUMNS, (at + 1) * COLUMNS)
        place = lax.broadcasted_iota(jnp.int32, (COLUMNS, head), 0) + at * COLUMNS
        across[:, chosen] = jnp.where(
            place < visible, values[chosen], jnp.zeros_like(values[chosen])
        ).T

    def visit(turn, carry):
        step = nth(turn)
        mixed_out[step] = attend(query_in[back(me, step)])

        @pl.when(turn == 0)
        def _():
            pl.semaphore_wait(barrier, HEADS - 1)

        send_mixed(step).start()
        return carry

    lax.fori_loop(0, HEADS - 1, visit, 0)
    mixed_in[me] = attend(query_in[me])

    per = COLUMNS // head
    halves = width // COLUMNS

    for copy in load_w:
        copy.wait()
    load_own.wait()
    for at in range(halves):
        gate[:, at * COLUMNS : (at + 1) * COLUMNS] = project(0, at)
        own_v = project(1, at).astype(jnp.bfloat16).astype(jnp.float32)
        own_k = project(2, at).astype(jnp.bfloat16).astype(jnp.float32)
        for number in range(per):
            part = slice(number * head, (number + 1) * head)
            query = own_query[at * per + number].astype(jnp.float32)
            weight = silu(jnp.sum(query * own_k[:, part], axis=-1, keepdims=True) * scale)
            weight = weight.astype(jnp.bfloat16).astype(jnp.float32)
            own[at * per + number] = weight * own_v[:, part]

    for step in ORDER:
        send_mixed(step).wait()

    total = jnp.zeros((slots, 1), jnp.float32)
    for number in range(HEADS):
        piece = mixed_in[number].astype(jnp.float32) + own[number]
        own[number] = piece
        total += jnp.sum(piece, axis=-1, keepdims=True)
    mean = total / width
    total = jnp.zeros((slots, 1), jnp.float32)
    for number in range(HEADS):
        piece = own[number] - mean
        total += jnp.sum(piece * piece, axis=-1, keepdims=True)
    factor = lax.rsqrt(total / width + 1e-05)
    for number in range(HEADS):
        part = slice(number * head, (number + 1) * head)
        normed[:, part] = (
            (own[number] - mean) * factor * gain_ref[:, part] * gate[:, part]
        ).astype(jnp.bfloat16)
    live = count - me * slots
    row = lax.broadcasted_iota(jnp.int32, (slots, COLUMNS), 0)
    for at in range(width // COLUMNS):
        columns = slice(at * COLUMNS, (at + 1) * COLUMNS)
        result = jnp.dot(normed[...], w_output[:, columns], preferred_element_type=jnp.float32)
        out_ref[:, columns] = jnp.where(row < live, result, 0.0).astype(jnp.bfloat16)


def score_call(tokens, prefix, query, own_query, w_uvqk, w_output, norm_gain, owner, counts, prefix_len):
    slots, width = tokens.shape
    head = width // HEADS
    length = prefix.shape[1]
    smem = pl.BlockSpec(memory_space=pltpu.SMEM)
    hbm = pl.BlockSpec(memory_space=pl.ANY)
    vmem = pl.BlockSpec(memory_space=pltpu.VMEM)
    bf16, f32 = jnp.bfloat16, jnp.float32
    return pl.pallas_call(
        score,
        out_shape=jax.ShapeDtypeStruct((slots, width), bf16),
        in_specs=[smem, smem, smem, vmem, vmem, hbm, hbm, hbm, vmem, vmem],
        out_specs=vmem,
        scratch_shapes=[
            pltpu.VMEM((length, head), bf16),
            pltpu.VMEM((length, head), bf16),
            pltpu.VMEM((head, length), bf16),
            pltpu.VMEM((3, width, width), bf16),
            pltpu.VMEM((HEADS, slots, head), bf16),
            pltpu.VMEM((HEADS, slots, head), bf16),
            pltpu.VMEM((HEADS, slots, head), bf16),
            pltpu.VMEM((slots, width), f32),
            pltpu.VMEM((HEADS, slots, head), f32),
            pltpu.VMEM((slots, width), bf16),
            pltpu.SemaphoreType.DMA((6,)),
            pltpu.SemaphoreType.DMA((HEADS,)),
            pltpu.SemaphoreType.DMA((HEADS,)),
        ],
        compiler_params=pltpu.CompilerParams(
            collective_id=0, has_side_effects=True, vmem_limit_bytes=48 * 1024 * 1024
        ),
        name="score",
    )(
        owner,
        counts,
        prefix_len,
        tokens,
        query,
        own_query,
        prefix,
        w_uvqk,
        w_output,
        norm_gain.reshape(1, width),
    )


def loads(shift, users, direct):
    per = 4
    ring = users // per
    leap = LEAP if shift * 2 > users else -LEAP
    carried = [0.0, 0.0]

    def carry(amount, distance):
        distance %= ring
        if distance * 2 == ring:
            carried[0] += amount * distance / 2
            carried[1] += amount * distance / 2
        elif distance * 2 < ring:
            carried[0] += amount * distance
        else:
            carried[1] += amount * (ring - distance)

    for share, distance in (
        (per - shift % per, shift // per),
        (shift % per, shift // per + 1),
    ):
        carry(share * direct, distance)
        carry(share * (PIECES - direct), leap)
        carry(share * (PIECES - direct), distance - leap)
    return max(carried) / (per * PIECES)


def plan(shift, users):
    leap = (LEAP if shift * 2 > users else -LEAP) * 4
    best = min(range(PIECES // 2, PIECES + 1), key=lambda direct: (loads(shift, users, direct), -direct))
    if loads(shift, users, PIECES) < 1.8 or loads(shift, users, best) > 0.9 * loads(shift, users, PIECES):
        best = PIECES
    return best, leap % users


def move(
    shift,
    users,
    rows_hbm,
    cache_hbm,
    w_hbm,
    tokens_hbm,
    prefix_hbm,
    query_hbm,
    own_query_hbm,
    tokens,
    staged_rows,
    staged_cache,
    kept,
    w_query,
    query_out,
    rows_send,
    rows_recv,
    relay_send,
    relay_recv,
    down_send,
    down_recv,
    along_send,
    along_recv,
    on_send,
    on_recv,
    query_send,
    query_recv,
    own_sem,
):
    me = lax.axis_index("helper")
    group = lax.axis_index("group")
    length, width = cache_hbm.shape[2:]
    slots = tokens.shape[0]
    head = width // HEADS
    piece = slots // PIECES
    direct, leap = plan(shift, users)
    relayed = PIECES - direct

    def at_group(steps):
        return lax.rem(group + steps % users, users)

    def remote(source, target, send, recv, **peer):
        return pltpu.make_async_remote_copy(
            src_ref=source,
            dst_ref=target,
            send_sem=send,
            recv_sem=recv,
            device_id=peer,
            device_id_type=MESH,
        )

    def piece_of(ref, number):
        return ref.at[pl.ds(pl.multiple_of(number * piece, piece), piece)]

    def columns_of(helper):
        return cache_hbm.at[0, :, :, pl.ds(pl.multiple_of(helper * head, head), head)]

    def place_of(helper):
        return prefix_hbm.at[:, pl.ds(pl.multiple_of(helper * length, length), length)]

    def send_rows(number):
        return remote(
            piece_of(rows_hbm.at[0], number),
            piece_of(tokens, number),
            rows_send.at[number],
            rows_recv.at[number],
            group=at_group(shift),
        )

    def send_relay(number):
        return remote(
            piece_of(rows_hbm.at[0], number),
            staged_rows.at[number - direct],
            relay_send.at[number - direct],
            relay_recv.at[number - direct],
            group=at_group(leap),
        )

    def send_relayed(number):
        return remote(
            staged_rows.at[number - direct],
            piece_of(tokens, number),
            rows_send.at[number],
            rows_recv.at[number],
            group=at_group(shift - leap),
        )

    partner = near(me, RUN)

    def send_down(step):
        target = place_of(me) if step == 0 else staged_cache.at[step - 1]
        return remote(
            columns_of(near(me, RUN + step)),
            target,
            down_send.at[step],
            down_recv.at[step],
            helper=partner,
        )

    def send_along(step):
        peer = near(me, step)
        return remote(
            columns_of(peer), place_of(me), along_send.at[step], along_recv.at[step], helper=peer
        )

    def send_on(step):
        return remote(
            staged_cache.at[step - 1],
            place_of(partner),
            on_send.at[step],
            on_recv.at[step],
            helper=near(me, step),
        )

    part = slots // GROUPS

    def send_query(step, number):
        peer = near(me, step)
        rows = pl.ds(pl.multiple_of(number * part, part), part)
        return remote(
            query_out.at[peer, rows],
            query_hbm.at[me, rows],
            query_send.at[step, number],
            query_recv.at[step, number],
            helper=peer,
        )

    keep = pltpu.make_async_copy(columns_of(me), kept, own_sem.at[0])
    put = pltpu.make_async_copy(kept, place_of(me), own_sem.at[1])
    load_w = pltpu.make_async_copy(w_hbm.at[:, pl.ds(2 * width, width)], w_query, own_sem.at[2])
    keep.start()
    load_w.start()
    if not shift:
        keep_rows = pltpu.make_async_copy(rows_hbm.at[0], tokens, own_sem.at[3])
        keep_rows.start()
    barrier = pltpu.get_barrier_semaphore()
    waits = HEADS - 1

    def greet(step, carry):
        pl.semaphore_signal(
            barrier, inc=1, device_id={"helper": near(me, step)}, device_id_type=MESH
        )
        return carry

    lax.fori_loop(1, HEADS, greet, 0)
    peers = [shift] if shift else []
    if relayed:
        peers += [leap, shift - leap]
    for steps in peers:
        for sign in (1, -1):
            pl.semaphore_signal(
                barrier, inc=1, device_id={"group": at_group(sign * steps)}, device_id_type=MESH
            )
            waits += 1
    pl.semaphore_wait(barrier, waits)

    def each(first, last, act):
        def body(number, carry):
            act(number)
            return carry

        if last > first:
            lax.fori_loop(first, last, body, 0)

    if shift:
        each(direct, PIECES, lambda number: send_relay(number).start())
        each(0, direct, lambda number: send_rows(number).start())
    send_down(2).start()
    for step in (1, 3, 2):
        send_along(step).start()
    for step in (1, 3, 0):
        send_down(step).start()

    def pass_rows(number):
        send_relay(number).wait_recv()
        send_relayed(number).start()

    for turn, step in enumerate((2, 1, 3)):
        send_down(step).wait_recv()
        send_on(step).start()
        if direct + turn < PIECES:
            pass_rows(direct + turn)
    each(direct + 3, PIECES, pass_rows)

    keep.wait()
    put.start()
    load_w.wait()
    if not shift:
        keep_rows.wait()
    wide = 2 * head

    def ask(number, carry):
        if shift:
            for turn in range(PIECES // GROUPS):
                send_rows(number * (PIECES // GROUPS) + turn).wait_recv()
        rows = pl.ds(pl.multiple_of(number * part, part), part)

        def columns(at, inner):
            block = silu(
                jnp.dot(
                    tokens[rows],
                    w_query[:, pl.ds(pl.multiple_of(at * wide, wide), wide)],
                    preferred_element_type=jnp.float32,
                )
            ).astype(jnp.bfloat16)
            query_out[2 * at, rows] = block[:, :head]
            query_out[2 * at + 1, rows] = block[:, head:]
            return inner

        lax.fori_loop(0, width // wide, columns, 0)
        each(1, HEADS, lambda step: send_query(step, number).start())
        return carry

    lax.fori_loop(0, GROUPS, ask, 0)
    put_rows = pltpu.make_async_copy(tokens, tokens_hbm, own_sem.at[4])
    put_query = pltpu.make_async_copy(query_out, own_query_hbm, own_sem.at[5])
    put_own = pltpu.make_async_copy(query_out.at[me], query_hbm.at[me], own_sem.at[6])
    for copy in (put_rows, put_query, put_own):
        copy.start()

    if shift:
        each(0, PIECES, lambda number: send_rows(number).wait_send())
        each(direct, PIECES, lambda number: send_relay(number).wait_send())
    send_down(0).wait()
    for step in (1, 2, 3):
        send_down(step).wait_send()
        send_along(step).wait()
        send_on(step).wait()
    for copy in (put, put_rows, put_query, put_own):
        copy.wait()

    def settle(number):
        each(1, HEADS, lambda step: send_query(step, number).wait())

    each(0, GROUPS, settle)


def move_call(shift, users, rows, cache, w_uvqk):
    slots, width = rows.shape[1:]
    length = cache.shape[2]
    head = width // HEADS
    hbm = pl.BlockSpec(memory_space=pl.ANY)
    bf16 = rows.dtype
    dma = pltpu.SemaphoreType.DMA
    return pl.pallas_call(
        functools.partial(move, shift, users),
        out_shape=(
            jax.ShapeDtypeStruct((slots, width), bf16),
            jax.ShapeDtypeStruct((2, HEADS * length, head), bf16),
            jax.ShapeDtypeStruct((HEADS, slots, head), bf16),
            jax.ShapeDtypeStruct((HEADS, slots, head), bf16),
        ),
        in_specs=[hbm, hbm, hbm],
        out_specs=(hbm, hbm, hbm, hbm),
        scratch_shapes=[
            pltpu.VMEM((slots, width), bf16),
            pltpu.VMEM((PIECES // 2, slots // PIECES, width), bf16),
            pltpu.VMEM((RUN - 1, 2, length, head), bf16),
            pltpu.VMEM((2, length, head), bf16),
            pltpu.VMEM((width, width), bf16),
            pltpu.VMEM((HEADS, slots, head), bf16),
            dma((PIECES,)),
            dma((PIECES,)),
            dma((PIECES // 2,)),
            dma((PIECES // 2,)),
            dma((RUN,)),
            dma((RUN,)),
            dma((RUN,)),
            dma((RUN,)),
            dma((RUN,)),
            dma((RUN,)),
            dma((HEADS, GROUPS)),
            dma((HEADS, GROUPS)),
            dma((7,)),
        ],
        compiler_params=pltpu.CompilerParams(collective_id=1 + shift, has_side_effects=True),
        name=f"move{shift}",
    )(rows, cache, w_uvqk)


def local(candidates, prefix_cache, w_uvqk, w_output, norm_gain, owner, counts, prefix_len):
    users = lax.axis_size("group")
    branches = [functools.partial(move_call, shift, users) for shift in range(users)]
    brought = lax.switch(owner[0], branches, candidates, prefix_cache, w_uvqk)
    return score_call(*brought, w_uvqk, w_output, norm_gain, owner, counts, prefix_len)[None]


def solution(mesh):
    in_specs = (
        P("group", "helper", None),
        P("group", None, "helper", None),
        P(),
        P(),
        P(),
        P(),
        P(),
        P(),
    )
    out_specs = P("group", "helper", None)
    return jax.shard_map(local, mesh=mesh, in_specs=in_specs, out_specs=out_specs, check_vma=False)
```
